32 devices in a mesh: dp: 4 (over y, z), fsdp: 8 (over x, core).
Axes of the slice: x: 4, y: 2, z: 2, core: 2. Of those that a mesh axis runs over, the one named last changes fastest.
The devices are a block of a 4x4x8 slice.
Arguments:
- prompts: bfloat16 [128, 512, 2048], P(('dp', 'fsdp')), parts along dimension 0
- ln1_gain: bfloat16 [2048], P('fsdp')
- ln1_bias: bfloat16 [2048], P('fsdp')
- w_qkv: bfloat16 [2048, 3, 32, 64], P('fsdp')
- b_qkv: bfloat16 [6144], P('fsdp')
- w_out: bfloat16 [2048, 2048], P('fsdp')
- b_out: bfloat16 [2048], P('fsdp')
- ln2_gain: bfloat16 [2048], P('fsdp')
- ln2_bias: bfloat16 [2048], P('fsdp')
- w_up: bfloat16 [2048, 8192], P('fsdp')
- b_up: bfloat16 [8192], P('fsdp')
- w_down: bfloat16 [8192, 2048], P('fsdp')
- b_down: bfloat16 [2048], P('fsdp')
Outputs:
- output 1: bfloat16 [128, 512, 2048], P(('dp', 'fsdp')), parts along dimension 0
- output 2: bfloat16 [128, 512, 32, 64], P(('dp', 'fsdp')), parts along dimension 0
- output 3: bfloat16 [128, 512, 32, 64], P(('dp', 'fsdp')), parts along dimension 0
There are 4 independent parts. The reference program is written for one: setup_inputs(seed, part) draws one part's arguments, and reference() takes and returns one part's arrays. A program takes and returns all parts, laid end to end along the dimension named above; an argument that names none is the same for every part.
All inputs are finite; a program needn't handle non-finite values.
Results may differ from the reference program's by a relative error of at most 0.00848424.
Values are sent between devices in bfloat16 or wider.
A program may use at most 768 MiB of HBM per device.

```python
import jax
import jax.numpy as jnp
from jax import lax

D = 2048
HEADS = 32
HEAD = 64
SEQ = 512
BATCH = 32
FFN = 4 * D
QBLOCK = min(SEQ, 256)
LN_EPS = 1e-5


def draw_normal(key, shape, scale, offset=0.0):
    return (offset + scale * jax.random.normal(key, shape, jnp.float32)).astype(jnp.bfloat16)


def setup_inputs(seed: int = 0, part: int = 0) -> dict:
    keys = jax.random.split(jax.random.key(seed), 13)
    return {
        'prompts': draw_normal(jax.random.fold_in(keys[0], part), (BATCH, SEQ, D), 1.0),
        'ln1_gain': draw_normal(keys[1], (D,), 0.3, 1.0),
        'ln1_bias': draw_normal(keys[2], (D,), 0.3),
        'w_qkv': draw_normal(keys[3], (D, 3, HEADS, HEAD), D ** -0.5),
        'b_qkv': draw_normal(keys[4], (3 * HEADS * HEAD,), 0.5),
        'w_out': draw_normal(keys[5], (HEADS * HEAD, D), (HEADS * HEAD) ** -0.5),
        'b_out': draw_normal(keys[6], (D,), 0.5),
        'ln2_gain': draw_normal(keys[7], (D,), 0.3, 1.0),
        'ln2_bias': draw_normal(keys[8], (D,), 0.3),
        'w_up': draw_normal(keys[9], (D, FFN), D ** -0.5),
        'b_up': draw_normal(keys[10], (FFN,), 0.5),
        'w_down': draw_normal(keys[11], (FFN, D), 1.5 * FFN ** -0.5),
        'b_down': draw_normal(keys[12], (D,), 0.5),
    }


def layer_norm(act, gain, shift):
    act_f32 = act.astype(jnp.float32)
    mean_val = jnp.mean(act_f32, axis=-1, keepdims=True)
    centered = act_f32 - mean_val
    var_val = jnp.mean(centered * centered, axis=-1, keepdims=True)
    normed = centered * lax.rsqrt(var_val + LN_EPS)
    return (normed * gain.astype(jnp.float32) + shift.astype(jnp.float32)).astype(jnp.bfloat16)


def reference(prompts, ln1_gain, ln1_bias, w_qkv, b_qkv, w_out, b_out, ln2_gain, ln2_bias, w_up, b_up, w_down, b_down):
    w_qkv_flat = w_qkv.reshape(D, 3 * HEADS * HEAD)
    key_pos = jnp.arange(SEQ)

    def one_prompt(prompt):
        normed1 = layer_norm(prompt, ln1_gain, ln1_bias)
        proj_qkv = jnp.dot(normed1, w_qkv_flat, preferred_element_type=jnp.float32)
        proj_qkv = (proj_qkv + b_qkv.astype(jnp.float32)).astype(jnp.bfloat16).reshape(SEQ, 3, HEADS, HEAD)
        keys_f32 = proj_qkv[:, 1].astype(jnp.float32)
        values_f32 = proj_qkv[:, 2].astype(jnp.float32)
        query_blocks = proj_qkv[:, 0].astype(jnp.float32).reshape(SEQ // QBLOCK, QBLOCK, HEADS, HEAD)

        def one_block(block_in):
            q_blk, blk_idx = block_in
            scores = jnp.einsum('qhe,khe->hqk', q_blk, keys_f32) * (HEAD ** -0.5)
            query_pos = blk_idx * QBLOCK + jnp.arange(QBLOCK)
            allowed = key_pos[None, :] <= query_pos[:, None]
            scores = jnp.where(allowed[None], scores, -jnp.inf)
            probs = jax.nn.softmax(scores, axis=-1).astype(jnp.bfloat16)
            context = jnp.einsum('hqk,khe->qhe', probs.astype(jnp.float32), values_f32)
            return context.astype(jnp.bfloat16)

        context = lax.map(one_block, (query_blocks, jnp.arange(SEQ // QBLOCK))).reshape(SEQ, HEADS * HEAD)
        attn_out = jnp.dot(context, w_out, preferred_element_type=jnp.float32)
        resid = (prompt.astype(jnp.float32) + attn_out + b_out.astype(jnp.float32)).astype(jnp.bfloat16)
        normed2 = layer_norm(resid, ln2_gain, ln2_bias)
        hidden = jnp.dot(normed2, w_up, preferred_element_type=jnp.float32) + b_up.astype(jnp.float32)
        hidden = jax.nn.gelu(hidden, approximate=True).astype(jnp.bfloat16)
        mlp_out = jnp.dot(hidden, w_down, preferred_element_type=jnp.float32)
        out_one = (resid.astype(jnp.float32) + mlp_out + b_down.astype(jnp.float32)).astype(jnp.bfloat16)
        return out_one, proj_qkv[:, 1], proj_qkv[:, 2]

    layer_out, k_cache, v_cache = lax.map(one_prompt, prompts)
    return layer_out, k_cache, v_cache
```

```python
import functools

import jax
import jax.numpy as jnp
from jax import lax
from jax.experimental import pallas as pl
from jax.experimental.pallas import tpu as pltpu
from jax.sharding import PartitionSpec as P

LN_EPS = 1e-5
LOG2E = 1.4426950408889634
MESH = pl.DeviceIdType.MESH
ANY = pl.BlockSpec(memory_space=pl.ANY)
SLOTS = 14
VMEM_LIMIT = 64 * 1024 * 1024 - 128 * 1024


def _nt(a, b):
    return lax.dot_general(a, b, (((1,), (1,)), ((), ())), preferred_element_type=jnp.float32)


class Where:
    def __init__(self, n):
        self.n = n
        self.g = lax.axis_index('dp')
        self.f = lax.axis_index('fsdp')
        self.p = lax.rem(self.g, 2)
        self.left = lax.rem(self.f + n - 2, n)
        self.right = lax.rem(self.f + 2, n)
        self.opp = lax.rem(self.f + n // 2, n)
        self.peer = self.f + 1 - 2 * lax.rem(self.f, 2)
        self.gz = self.g + 1 - 2 * self.p

    def greet(self, everyone):
        bar = pltpu.get_barrier_semaphore()
        if everyone:
            ids = [(self.g, lax.rem(self.f + r, self.n)) for r in range(1, self.n)]
        else:
            ids = [(self.g, self.left), (self.g, self.right), (self.g, self.peer)]
        ids.append((self.gz, self.f))
        for d in ids:
            pl.semaphore_signal(bar, inc=1, device_id=d, device_id_type=MESH)
        pl.semaphore_wait(bar, len(ids))


class Gather:
    def __init__(self, w, total, src, dst, send, recv):
        self.w, self.total, self.src, self.dst, self.send, self.recv = w, total, src, dst, send, recv

    def copy(self, c, k):
        w, p = self.w, self.w.p
        right, left, peer, pair = (w.g, w.right), (w.g, w.left), (w.g, w.peer), (w.gz, w.f)
        if k <= 2:
            to = (right, left, peer)[k]
            q, n = (p, 3) if k < 2 else (0, 4)
            a, b = self.src(c, q, n), self.dst(c, w.f, q, n)
        else:
            dev, q, n, to = {
                3: (w.left, 2 * p, 1, right),
                4: (w.right, 2 * p + 1, 1, left),
                5: (w.left, 3 * p, 1, pair),
                6: (w.right, 3 * p, 1, pair),
                7: (w.opp, 2 * p, 2, pair),
                8: (w.left, p, 3, peer),
                9: (w.right, p, 3, peer),
                10: (w.opp, 2 * p, 2, peer),
                11: (w.left, 3 - 3 * p, 1, peer),
                12: (w.right, 3 - 3 * p, 1, peer),
                13: (w.opp, 2 - 2 * p, 2, peer),
            }[k]
            a = b = self.dst(c, dev, q, n)
        return pltpu.make_async_remote_copy(
            src_ref=a, dst_ref=b, send_sem=self.send.at[c, k], recv_sem=self.recv.at[c, k], device_id=to, device_id_type=MESH)

    def start(self, c, ks):
        for k in ks:
            self.copy(c, k).start()

    def arrive(self, c, ks):
        for k in ks:
            self.copy(c, k).wait_recv()

    def prelude(self):
        for c in range(min(2, self.total)):
            self.start(c, (0, 1, 2))

    def _when(self, c, fn):
        if isinstance(c, int):
            if 0 <= c < self.total:
                fn(c)
        else:
            pl.when(jnp.logical_and(c >= 0, c < self.total))(lambda: fn(c))

    def tick(self, t):
        def done(c):
            self.arrive(c, (2, 8, 9, 10, 11, 12, 13))
            for k in range(SLOTS):
                self.copy(c, k).wait_send()

        def far(c):
            self.arrive(c, (5, 6, 7))
            self.start(c, (11, 12, 13))

        def mid(c):
            self.arrive(c, (3, 4))
            self.start(c, (7, 10))

        def near(c):
            self.arrive(c, (0, 1))
            self.start(c, (3, 4, 5, 6, 8, 9))

        self._when(t - 3, done)
        self._when(t - 2, far)
        self._when(t - 1, mid)
        self._when(t, near)
        nxt = t + 2
        if isinstance(t, int):
            if nxt < self.total:
                self.start(nxt, (0, 1, 2))
        else:
            pl.when(nxt < self.total)(lambda: self.start(nxt, (0, 1, 2)))

    @property
    def ticks(self):
        return self.total + 3


def _sems(n):
    return [pltpu.SemaphoreType.DMA((n, SLOTS)), pltpu.SemaphoreType.DMA((n, SLOTS))]


def _row_src(refs_cols):
    def src(c, q, n):
        ref, c0, width = refs_cols[c]
        u = width // 4
        return ref.at[:, pl.ds(pl.multiple_of(c0 + q * u, 128), n * u)]

    return src


def _row_dst(bufs, depth):
    def dst(c, dev, q, n):
        u = bufs[c].shape[1] // 4
        return bufs[c].at[pl.ds(pl.multiple_of(dev * depth, depth), depth), pl.ds(pl.multiple_of(q * u, 128), n * u)]

    return dst


def _ln(xf, gain, shift):
    mean = jnp.mean(xf, axis=-1, keepdims=True)
    cen = xf - mean
    var = jnp.mean(cen * cen, axis=-1, keepdims=True)
    return (cen * lax.rsqrt(var + LN_EPS) * gain + shift).astype(jnp.bfloat16)


def qkv_kernel(cfg, x_ref, w_ref, small_ref, qt, kt, vt, small_out, wbuf, hbuf, xbuf, sbuf, bias, obuf, xsem, ssend, srecv, lsem, osem, send, recv):
    n, rows, batch, seq, nchunks, brow = cfg
    w = Where(n)
    d_model = hbuf.shape[1]
    depth = d_model // n
    w.greet(True)

    def src(c, q, m):
        return w_ref.at[pl.ds(pl.multiple_of(c * rows + q * (rows // 4), 16), m * (rows // 4)), :]

    def dst(c, dev, q, m):
        return wbuf.at[pl.ds(pl.multiple_of(c * rows + q * (rows // 4), 16), m * (rows // 4)), pl.ds(pl.multiple_of(dev * depth, 128), depth)]

    ga = Gather(w, nchunks, src, dst, send, recv)

    def lanes(dev):
        return sbuf.at[:, pl.ds(pl.multiple_of(dev * depth, 128), depth)]

    smalls = []
    for r in range(1, n):
        cp = pltpu.make_async_remote_copy(
            src_ref=small_ref, dst_ref=lanes(w.f), send_sem=ssend.at[r], recv_sem=srecv.at[r],
            device_id=(w.g, lax.rem(w.f + r, n)), device_id_type=MESH)
        cp.start()
        smalls.append(cp)
    ga.prelude()
    own_small = pltpu.make_async_copy(small_ref, lanes(w.f), lsem.at[0])
    own_small.start()
    own_w = pltpu.make_async_copy(w_ref, wbuf.at[:, pl.ds(pl.multiple_of(w.f * depth, 128), depth)], lsem.at[1])
    own_w.start()

    blk = xbuf.shape[1]
    nblk = hbuf.shape[0] // blk

    def xcopy(i, slot):
        return pltpu.make_async_copy(x_ref.at[pl.ds(pl.multiple_of(i * blk, blk), blk), :], xbuf.at[slot], xsem.at[slot])

    xcopy(0, 0).start()
    own_small.wait()
    for cp in smalls:
        cp.wait()
    put_small = pltpu.make_async_copy(sbuf, small_out, lsem.at[2])
    put_small.start()
    gain = sbuf[pl.ds(0, 1), :].astype(jnp.float32)
    shift = sbuf[pl.ds(1, 1), :].astype(jnp.float32)

    def ln_step(i, _):
        slot = lax.rem(i, 2)

        @pl.when(i + 1 < nblk)
        def _():
            xcopy(i + 1, 1 - slot).start()

        xcopy(i, slot).wait()
        hbuf[pl.ds(pl.multiple_of(i * blk, blk), blk), :] = _ln(xbuf[slot].astype(jnp.float32), gain, shift)
        return 0

    lax.fori_loop(0, nblk, ln_step, 0)
    own_w.wait()

    total_rows = nchunks * rows
    per = total_rows // n // depth
    for m in range(n * per):
        j, r = m // per, m % per
        row = sbuf[pl.ds(brow + r, 1), pl.ds(j * depth, depth)].astype(jnp.float32)
        bias[pl.ds(m * depth, depth), :] = jnp.broadcast_to(row, (128, depth)).T

    def ocopy(ref, c_in, b, slot):
        return pltpu.make_async_copy(obuf.at[slot], ref.at[b, pl.ds(pl.multiple_of(c_in * rows, rows), rows), :], osem.at[slot])

    per_out = nchunks // 3

    def chunk_step(i, _):
        ga.tick(i)
        c = i - 3

        @pl.when(c >= 0)
        def _():
            def one(b, _):
                slot = lax.rem(b, 2)

                @pl.when(jnp.logical_or(c > 0, b >= 2))
                def _():
                    ocopy(qt, 0, 0, slot).wait()

                sub = 256
                for s in range(rows // sub):
                    r0 = pl.multiple_of(c * rows + s * sub, sub)
                    acc = _nt(wbuf[pl.ds(r0, sub), :], hbuf[pl.ds(pl.multiple_of(b * seq, seq), seq), :])
                    bcol = bias[pl.ds(r0, sub), :]
                    acc = acc + jnp.concatenate([bcol] * (seq // 128), axis=1)
                    obuf[slot, pl.ds(s * sub, sub), :] = acc.astype(jnp.bfloat16)
                c_in = lax.rem(c, per_out)
                for o, ref in enumerate((qt, kt, vt)):
                    @pl.when(lax.div(c, per_out) == o)
                    def _():
                        ocopy(ref, c_in, b, slot).start()
                return 0

            lax.fori_loop(0, batch, one, 0)

        return 0

    lax.fori_loop(0, ga.ticks, chunk_step, 0)
    for slot in range(2):
        ocopy(qt, 0, 0, slot).wait()
    put_small.wait()


def qkv_call(n, x2, wt, small, batch, seq, brow):
    tokens, d_model = x2.shape
    total = wt.shape[0]
    rows = 1024
    nchunks = total // rows
    cfg = (n, rows, batch, seq, nchunks, brow)
    o = jax.ShapeDtypeStruct((batch, total // 3, seq), jnp.bfloat16)
    return pl.pallas_call(
        functools.partial(qkv_kernel, cfg),
        out_shape=(o, o, o, jax.ShapeDtypeStruct((small.shape[0], d_model), jnp.bfloat16)),
        in_specs=[ANY] * 3,
        out_specs=(ANY,) * 4,
        scratch_shapes=[
            pltpu.VMEM((total, d_model), jnp.bfloat16),
            pltpu.VMEM((tokens, d_model), jnp.bfloat16),
            pltpu.VMEM((2, 256, d_model), jnp.bfloat16),
            pltpu.VMEM((small.shape[0], d_model), jnp.bfloat16),
            pltpu.VMEM((total, 128), jnp.float32),
            pltpu.VMEM((2, rows, seq), jnp.bfloat16),
            pltpu.SemaphoreType.DMA((2,)),
            pltpu.SemaphoreType.DMA((n,)),
            pltpu.SemaphoreType.DMA((n,)),
            pltpu.SemaphoreType.DMA((3,)),
            pltpu.SemaphoreType.DMA((2,)),
        ] + _sems(nchunks),
        compiler_params=pltpu.CompilerParams(collective_id=1, has_side_effects=True, vmem_limit_bytes=VMEM_LIMIT),
        name='qkv',
    )(x2, wt, small)


def attention_kernel(cfg, qt, kt, vt, *rest):
    n, head, gather_of, nref, nbuf, every = cfg
    wrefs, ctx, bufs = rest[:nref], rest[nref], rest[nref + 1:nref + 1 + nbuf]
    send, recv = rest[nref + 1 + nbuf:]
    step = pl.program_id(0) * pl.num_programs(1) + pl.program_id(1)
    w = Where(n)
    ga = gather_of(w, wrefs, bufs, send, recv)

    @pl.when(step == 0)
    def _():
        w.greet(False)
        ga.prelude()

    for t in range(ga.ticks):
        @pl.when(step == min((t + 1) * every, pl.num_programs(0) * pl.num_programs(1) - 1))
        def _():
            ga.tick(t)

    rows, seq = qt.shape[1], qt.shape[2]
    half = seq // 2
    c = (head ** -0.5) * LOG2E
    kpos = lax.broadcasted_iota(jnp.int32, (half, half), 0)
    qpos = lax.broadcasted_iota(jnp.int32, (half, half), 1)
    allowed = kpos <= qpos
    tn = (((0,), (0,)), ((), ()))
    for pair in range(rows // (2 * head)):
        outs = []
        for hh in range(2):
            r = pl.ds((2 * pair + hh) * head, head)
            q, k, v = qt[0, r, :], kt[0, r, :], vt[0, r, :]
            k_t = k.T
            s0 = jnp.dot(k_t[:half], q[:, :half], preferred_element_type=jnp.float32)
            s0 = jnp.where(allowed, s0, -jnp.inf)
            m0 = jnp.max(s0, axis=0, keepdims=True)
            e0 = jnp.exp2((s0 - m0) * c)
            p0 = (e0 * (1.0 / jnp.sum(e0, axis=0, keepdims=True))).astype(jnp.bfloat16)
            o0 = jnp.dot(v[:, :half], p0, preferred_element_type=jnp.float32)
            s1 = jnp.dot(k_t[:half], q[:, half:], preferred_element_type=jnp.float32)
            s2 = jnp.dot(k_t[half:], q[:, half:], preferred_element_type=jnp.float32)
            s2 = jnp.where(allowed, s2, -jnp.inf)
            m1 = jnp.maximum(jnp.max(s1, axis=0, keepdims=True), jnp.max(s2, axis=0, keepdims=True))
            e1 = jnp.exp2((s1 - m1) * c)
            e2 = jnp.exp2((s2 - m1) * c)
            inv = 1.0 / (jnp.sum(e1, axis=0, keepdims=True) + jnp.sum(e2, axis=0, keepdims=True))
            p1 = jnp.concatenate([(e1 * inv).astype(jnp.bfloat16), (e2 * inv).astype(jnp.bfloat16)], axis=0)
            o1 = jnp.dot(v, p1, preferred_element_type=jnp.float32)
            outs.append(jnp.concatenate([o0, o1], axis=1))
        o = jnp.concatenate(outs, axis=0)
        ctx[:, pl.ds(pair * 2 * head, 2 * head)] = o.T.astype(jnp.bfloat16)


def attention_call(n, qt, kt, vt, head, gather_of, wrefs, bufs, total, every):
    batch, d_model, seq = qt.shape
    rows = 256
    grid = (batch, d_model // rows)
    spec = pl.BlockSpec((1, rows, seq), lambda b, h: (b, h, 0))
    nref, nbuf = len(wrefs), len(bufs)
    out = pl.pallas_call(
        functools.partial(attention_kernel, (n, head, gather_of, nref, nbuf, every)),
        grid=grid,
        out_shape=(jax.ShapeDtypeStruct((batch * seq, d_model), jnp.bfloat16),) + tuple(bufs),
        in_specs=[spec] * 3 + [ANY] * nref,
        out_specs=(pl.BlockSpec((seq, rows), lambda b, h: (b, h)),) + (ANY,) * nbuf,
        scratch_shapes=_sems(total),
        compiler_params=pltpu.CompilerParams(collective_id=2, has_side_effects=True, vmem_limit_bytes=VMEM_LIMIT),
        name='attention',
    )(qt, kt, vt, *wrefs)
    return out[0], list(out[1:])


def load_parts(n, f, buf, own, dst, sem, start):
    depth = own.shape[0]
    if not start:
        pltpu.make_async_copy(buf, dst, sem).wait()
        return
    for r in range(n):
        dev = lax.rem(f + r, n)
        rows = pl.ds(pl.multiple_of(dev * depth, depth), depth)
        pltpu.make_async_copy(own if r == 0 else buf.at[rows, :], dst.at[rows, :], sem).start()


def out_kernel(cfg, ctx, x, small, wo_own, *rest):
    n, nwo, gather_of, nref, nbuf, every, rows_of = cfg
    wo, rest = rest[:nwo], rest[nwo:]
    wrefs, (x1, h2), bufs = rest[:nref], rest[nref:nref + 2], rest[nref + 2:nref + 2 + nbuf]
    wv, lsem, send, recv = rest[nref + 2 + nbuf:]
    i = pl.program_id(0)
    w = Where(n)
    ga = gather_of(w, wrefs, bufs, send, recv)
    width = wv.shape[1] // nwo

    @pl.when(i == 0)
    def _():
        w.greet(False)
        ga.prelude()
        for start in (True, False):
            for c in range(nwo):
                cols = pl.ds(c * width, width)
                load_parts(n, w.f, wo[c], wo_own.at[:, cols], wv.at[:, cols], lsem.at[c], start)

    for t in range(ga.ticks):
        @pl.when(i == min((t + 1) * every, pl.num_programs(0) - 1))
        def _():
            ga.tick(t)

    bo, g2, b2 = (small[pl.ds(r, 1), :].astype(jnp.float32) for r in rows_of)
    acc = jnp.dot(ctx[...], wv[...], preferred_element_type=jnp.float32)
    y = (x[...].astype(jnp.float32) + acc + bo).astype(jnp.bfloat16)
    x1[...] = y
    h2[...] = _ln(y.astype(jnp.float32), g2, b2)


def out_call(n, ctx, x2, small, wo_own, wo, gather_of, wrefs, bufs, total, every, rows_of):
    tokens, d_model = x2.shape
    m = 256
    blk = pl.BlockSpec((m, d_model), lambda i: (i, 0))
    o = jax.ShapeDtypeStruct((tokens, d_model), jnp.bfloat16)
    nref, nbuf = len(wrefs), len(bufs)
    out = pl.pallas_call(
        functools.partial(out_kernel, (n, len(wo), gather_of, nref, nbuf, every, rows_of)),
        grid=(tokens // m,),
        out_shape=(o, o) + tuple(bufs),
        in_specs=[blk, blk, pl.BlockSpec(small.shape, lambda i: (0, 0)), ANY] + [ANY] * (len(wo) + nref),
        out_specs=(blk, blk) + (ANY,) * nbuf,
        scratch_shapes=[pltpu.VMEM((ctx.shape[1], d_model), jnp.bfloat16), pltpu.SemaphoreType.DMA((len(wo),))] + _sems(total),
        compiler_params=pltpu.CompilerParams(collective_id=3, has_side_effects=True, vmem_limit_bytes=VMEM_LIMIT),
        name='outproj',
    )(ctx, x2, small, wo_own, *wo, *wrefs)
    return out[0], out[1], list(out[2:])


def mm_kernel(cfg, a, bias, res, own, *rest):
    n, epilogue, npre, nnew, gather_of, nref, nbuf, tick_at, ready_at = cfg
    pre, rest = rest[:npre], rest[npre:]
    wrefs, rest = rest[:nref], rest[nref:]
    out, bufs = rest[0], rest[1:1 + nbuf]
    wv, lsem, send, recv = rest[1 + nbuf:]
    chunks = list(pre) + list(bufs[:nnew])
    j, i = pl.program_id(0), pl.program_id(1)
    ni = pl.num_programs(1)
    step = j * ni + i
    w = Where(n)
    ga = gather_of(w, wrefs, bufs, send, recv) if gather_of is not None else None
    width = wv.shape[2]

    def load(c, start):
        load_parts(n, w.f, chunks[c], own.at[:, pl.ds(c * width, width)], wv.at[c % 2], lsem.at[c % 2], start)

    @pl.when(step == 0)
    def _():
        load(0, True)
        if ga is not None:
            w.greet(False)
            ga.prelude()

    if ga is not None:
        for t in range(ga.ticks):
            @pl.when(step == tick_at[t])
            def _():
                ga.tick(t)

    for c in range(len(chunks)):
        @pl.when(jnp.logical_and(j == c, i == 0))
        def _():
            load(c, False)

        if c + 1 < len(chunks):
            @pl.when(jnp.logical_and(j == c, i == ni - 1))
            def _():
                load(c + 1, True)

    acc = jnp.dot(a[...], wv[lax.rem(j, 2)], preferred_element_type=jnp.float32)
    acc = acc + bias[...].astype(jnp.float32)
    if epilogue == 'gelu':
        out[...] = jax.nn.gelu(acc, approximate=True).astype(jnp.bfloat16)
    else:
        out[...] = (res[...].astype(jnp.float32) + acc).astype(jnp.bfloat16)


def mm_call(n, name, cid, a, bias, res, own, pre, new, m, width, epilogue, gather_of, wrefs, bufs, total, tick_at):
    tokens, k = a.shape
    nout = own.shape[1]
    nj, ni = nout // width, tokens // m
    comm = gather_of is not None
    nref, nbuf = len(wrefs), len(bufs)
    res_spec = pl.BlockSpec((m, width), lambda j, i: (i, j)) if epilogue != 'gelu' else pl.BlockSpec((16, 128), lambda j, i: (0, 0))
    out = pl.pallas_call(
        functools.partial(mm_kernel, (n, epilogue, len(pre), new, gather_of, nref, nbuf, tick_at, None)),
        grid=(nj, ni),
        out_shape=(jax.ShapeDtypeStruct((tokens, nout), jnp.bfloat16),) + tuple(bufs),
        in_specs=[pl.BlockSpec((m, k), lambda j, i: (i, 0)), pl.BlockSpec((1, width), lambda j, i: (0, j)), res_spec, ANY] + [ANY] * (len(pre) + nref),
        out_specs=(pl.BlockSpec((m, width), lambda j, i: (i, j)),) + (ANY,) * nbuf,
        scratch_shapes=[pltpu.VMEM((2, k, width), jnp.bfloat16), pltpu.SemaphoreType.DMA((2,))] + _sems(max(total, 1)),
        compiler_params=pltpu.CompilerParams(collective_id=cid, has_side_effects=True, vmem_limit_bytes=VMEM_LIMIT) if comm else pltpu.CompilerParams(vmem_limit_bytes=VMEM_LIMIT),
        name=name,
    )(a, bias, res, own, *pre, *wrefs)
    return out[0], list(out[1:])


def solution(mesh):
    batch_axes = ('dp', 'fsdp')
    n = mesh.shape['fsdp']

    def local_layer(prompts, ln1_gain, ln1_bias, w_qkv, b_qkv, w_out, b_out, ln2_gain, ln2_bias, w_up, b_up, w_down, b_down):
        batch, seq, d_model = prompts.shape
        heads, head = w_qkv.shape[2], w_qkv.shape[3]
        ffn = w_up.shape[1]
        depth = d_model // n
        x2 = prompts.reshape(batch * seq, d_model)
        wt = w_qkv.transpose(1, 2, 3, 0).reshape(3 * heads * head, depth)

        vecs = [ln1_gain, ln1_bias, b_out, ln2_gain, ln2_bias, b_down, b_qkv, b_up]
        small = jnp.concatenate([v.reshape(-1, depth) for v in vecs], axis=0)
        brow = 6
        urow = brow + b_qkv.shape[0] // depth
        nrow = urow + b_up.shape[0] // depth
        small = jnp.pad(small, ((0, -nrow % 16), (0, 0)))

        qt, kt, vt, small = qkv_call(n, x2, wt, small, batch, seq, brow)

        cu = 1024
        cd = d_model // 4
        up_buf = jax.ShapeDtypeStruct((d_model, cu), jnp.bfloat16)
        dn_buf = jax.ShapeDtypeStruct((ffn, cd), jnp.bfloat16)

        def up_gather(first, count):
            def make(w, wrefs, bufs, send, recv):
                return Gather(w, count, _row_src([(wrefs[0], (first + c) * cu, cu) for c in range(count)]), _row_dst(bufs, depth), send, recv)
            return make

        n2, n3 = 3, 2
        nwo = d_model // cu

        def attn_gather(w, wrefs, bufs, send, recv):
            parts = [(wrefs[0], c * cu, cu) for c in range(nwo)] + [(wrefs[1], c * cu, cu) for c in range(n2)]
            return Gather(w, nwo + n2, _row_src(parts), _row_dst(bufs, depth), send, recv)

        ctx, got = attention_call(n, qt, kt, vt, head, attn_gather, [w_out, w_up], [up_buf] * (nwo + n2), nwo + n2, 3)
        wo, up = got[:nwo], got[nwo:]
        x1, h2, got = out_call(n, ctx, x2, small, w_out, wo, up_gather(n2, n3), [w_up], [up_buf] * n3, n3, 1, (2, 3, 4))
        up += got

        nup = ffn // cu
        left = nup - n2 - n3
        ndn = d_model // cd
        nd4 = 2

        def dn_parts(wref, first, count, bufs):
            u = wref.shape[0] // 4
            kd = wref.shape[0]

            def src(c, q, m):
                return wref.at[pl.ds(pl.multiple_of(q * u, u), m * u), pl.ds((first + c) * cd, cd)]

            def dst(c, dev, q, m):
                return bufs[c].at[pl.ds(pl.multiple_of(dev * kd + q * u, u), m * u), :]

            return src, dst

        def mlp_gather(w, wrefs, bufs, send, recv):
            usrc = _row_src([(wrefs[0], (n2 + n3 + c) * cu, cu) for c in range(left)])
            udst = _row_dst(bufs[:left], depth)
            dsrc, ddst = dn_parts(wrefs[1], 0, nd4, bufs[left:])
            return Gather(
                w, left + nd4,
                lambda c, q, m: usrc(c, q, m) if c < left else dsrc(c - left, q, m),
                lambda c, dev, q, m: udst(c, dev, q, m) if c < left else ddst(c - left, dev, q, m),
                send, recv)

        def down_gather(w, wrefs, bufs, send, recv):
            src, dst = dn_parts(wrefs[0], nd4, ndn - nd4, bufs)
            return Gather(w, ndn - nd4, src, dst, send, recv)

        b_up_row = small[urow:urow + ffn // d_model].reshape(ffn // d_model, n, depth).transpose(1, 0, 2).reshape(1, ffn)
        b_dn_row = small[5:6]
        hid, got = mm_call(
            n, 'mlpup', 4, h2, b_up_row, h2, w_up, up, left, 512, cu, 'gelu', mlp_gather, [w_up, w_down],
            [up_buf] * left + [dn_buf] * nd4, left + nd4, [4, 8, 12, 16, 19, 23, 27, 31])
        dn = got[left:]
        y, _ = mm_call(
            n, 'mlpdown', 5, hid, b_dn_row, x1, w_down, dn, ndn - nd4, 512, cd, 'residual', down_gather, [w_down],
            [dn_buf] * (ndn - nd4), ndn - nd4, [2, 4, 6, 7, 11])

        def cache(t):
            return t.reshape(batch, heads, head, seq).transpose(0, 3, 1, 2)

        return y.reshape(batch, seq, d_model), cache(kt), cache(vt)

    weight_spec = P('fsdp')
    return jax.shard_map(local_layer, mesh=mesh, in_specs=(P(batch_axes),) + (weight_spec,) * 12, out_specs=(P(batch_axes), P(batch_axes), P(batch_axes)), check_vma=False)
```
